32 devices in a mesh: rep: 1 (over z), dp: 32 (over x, y, core).
Axes of the slice: x: 4, y: 4, z: 1, core: 2. Of those that a mesh axis runs over, the one named last changes fastest.
The devices are a block of a 4x4x8 slice.
Arguments:
- g_w_gate: bfloat16 [32, 2, 1280, 4480], P(('rep', 'dp'))
- g_w_up: bfloat16 [32, 2, 1280, 4480], P(('rep', 'dp'))
- g_w_down: bfloat16 [32, 2, 4480, 1280], P(('rep', 'dp'))
- w_gate: bfloat16 [2, 1280, 4480], replicated
- w_up: bfloat16 [2, 1280, 4480], replicated
- w_down: bfloat16 [2, 4480, 1280], replicated
- m_w_gate: float32 [2, 1280, 4480], P(None, 'dp')
- m_w_up: float32 [2, 1280, 4480], P(None, 'dp')
- m_w_down: float32 [2, 4480, 1280], P(None, 'dp')
- v_w_gate: float32 [2, 1280, 4480], P(None, 'dp')
- v_w_up: float32 [2, 1280, 4480], P(None, 'dp')
- v_w_down: float32 [2, 4480, 1280], P(None, 'dp')
Outputs:
- output 1: bfloat16 [2, 1280, 4480], P('rep')
- output 2: bfloat16 [2, 1280, 4480], P('rep')
- output 3: bfloat16 [2, 4480, 1280], P('rep')
- output 4: float32 [2, 1280, 4480], P('rep', 'dp')
- output 5: float32 [2, 1280, 4480], P('rep', 'dp')
- output 6: float32 [2, 4480, 1280], P('rep', 'dp')
- output 7: float32 [2, 1280, 4480], P('rep', 'dp')
- output 8: float32 [2, 1280, 4480], P('rep', 'dp')
- output 9: float32 [2, 4480, 1280], P('rep', 'dp')
All inputs are finite; a program needn't handle non-finite values.
Results may differ from the reference program's by a relative error of at most 0.022.
Values are sent between devices in bfloat16 or wider.
A program may use at most 768 MiB of HBM per device.

```python
import jax
import jax.numpy as jnp
from jax import lax

DEVICES = 32
D = 1280
FF = 4480
LAYERS = 2
NAMES = ("w_gate", "w_up", "w_down")
SHAPES = {"w_gate": (LAYERS, D, FF), "w_up": (LAYERS, D, FF), "w_down": (LAYERS, FF, D)}


def setup_inputs(seed: int = 0, part: int = 0) -> dict:
    kz, *keys = jax.random.split(jax.random.key(seed), 1 + 5 * len(NAMES))
    loud = 2.0 ** jax.random.uniform(kz, (), jnp.float32, -1.0, 1.0)
    drawn = {}
    for name, key, both in zip(NAMES, keys[:3], keys[3:6], strict=True):
        own = jax.random.normal(jax.random.fold_in(key, part), (DEVICES, *SHAPES[name]), jnp.float32)
        shared = jax.random.normal(jax.random.fold_in(both, part), SHAPES[name], jnp.float32)
        drawn["g_" + name] = (loud * (0.7 * shared / DEVICES + 0.7 * own * DEVICES**-0.5)).astype(jnp.bfloat16)
    for name, key in zip(NAMES, keys[6:9], strict=True):
        drawn[name] = (jax.random.normal(key, SHAPES[name], jnp.float32) * SHAPES[name][1] ** -0.5).astype(jnp.bfloat16)
    for name, key in zip(NAMES, keys[9:12], strict=True):
        drawn["m_" + name] = loud * 0.5 * jax.random.normal(key, SHAPES[name], jnp.float32)
    for name, key in zip(NAMES, keys[12:15], strict=True):
        drawn["v_" + name] = loud * loud * jax.random.uniform(key, SHAPES[name], jnp.float32, 0.5, 1.5)
    return drawn


def adamw(w, m, v, g):
    m = 0.9 * m + 0.1 * g
    v = 0.95 * v + 0.05 * g * g
    step = m * lax.rsqrt(v + 1e-8) + 0.1 * w
    return (w - 0.02 * step).astype(jnp.bfloat16), m, v


def reference(g_w_gate, g_w_up, g_w_down, w_gate, w_up, w_down, m_w_gate, m_w_up, m_w_down, v_w_gate, v_w_up, v_w_down):
    def total(terms):
        return lax.scan(lambda so_far, term: (so_far + term.astype(jnp.float32), None), jnp.zeros(terms.shape[1:], jnp.float32), terms)[0]

    gradients = [total(terms).astype(jnp.bfloat16).astype(jnp.float32) for terms in (g_w_gate, g_w_up, g_w_down)]
    new = [
        adamw(w.astype(jnp.float32), m, v, g)
        for w, m, v, g in zip((w_gate, w_up, w_down), (m_w_gate, m_w_up, m_w_down), (v_w_gate, v_w_up, v_w_down), gradients, strict=True)
    ]
    return tuple(one[which] for which in range(3) for one in new)
```

```python
import functools
import math

import jax
import jax.numpy as jnp
from jax import lax
from jax.experimental import pallas as pl
from jax.experimental.pallas import tpu as pltpu
from jax.sharding import PartitionSpec as P

MESH = pl.DeviceIdType.MESH
F32, BF16 = jnp.float32, jnp.bfloat16
CORES, SIDE = 2, 4
WEIGHTS = 3
ROWS, COLS = 40, 640
LAG = (0, 1, 2, 3, 4)
SLOTS = LAG[4] + LAG[2] + 2
HELD = LAG[4] + 2
SENT = 3
AHEAD = 3


def fused(pieces, *refs):
    (gd, gg, gu, wd, wg, wu, md, vd, mg, vg, mu, vu, whole, sum_d, sum_g, sum_u, theirs,
     own, par, r1, r2, u1, u2, s1, s2, t1, t2, total, new, got3, gotm, put3, putm, newm, mbd, vbd, wb3, wbm, mbg, vbg, wbg,
     sem_load, sem_swap_s, sem_swap_r, sem_r1, sem_r2, sem_u1, sem_u2, sem_s1, sem_s2, sem_t1, sem_t2,
     sem_m, sem_out, sem_xs, sem_xr, sem_own, sem_gs, sem_gr, sem_os, sem_or) = refs
    count = WEIGHTS * pieces
    me = lax.axis_index("dp")
    x, y, c = me // (CORES * SIDE), (me // CORES) % SIDE, me % CORES
    other = 1 - c

    def dev(x, y, c):
        return ((x % SIDE) * SIDE + y % SIDE) * CORES + c

    partner = dev(x, y, other)
    place = ((x, y), (y, x))

    def dev_i(t, d):
        return dev(x + d, y, c) if t == 0 else dev(x, y + d, c)

    def dev_j(t, d):
        return dev_i(1 - t, d)

    def at(t, i, j):
        return (i % SIDE, j % SIDE) if t == 0 else (j % SIDE, i % SIDE)

    def send(src, dst, ssem, rsem, to):
        return pltpu.make_async_remote_copy(src_ref=src, dst_ref=dst, send_sem=ssem, recv_sem=rsem, device_id={"dp": to}, device_id_type=MESH)

    def wait(ref, sem):
        pltpu.make_async_copy(ref, ref, sem).wait()

    def of_weight(q, do):
        for w in range(WEIGHTS):
            @pl.when(q // pieces == w)
            def _(w=w):
                do(w, q % pieces)

    def term(w, t, p, core):
        if w == 0:
            return gd.at[t, :, :, pl.ds(pl.multiple_of(p * ROWS, 8), ROWS), pl.ds(pl.multiple_of(core * COLS, 128), COLS)]
        return (gg, gu)[w - 1].at[t, :, :, core, :, pl.ds(pl.multiple_of(p * COLS, 128), COLS)]

    def swap(q):
        def do(w, p):
            for t in range(2):
                send(term(w, t, p, other), theirs.at[q, t], sem_swap_s.at[t], sem_swap_r.at[q, t], partner).start()
        of_weight(q, do)

    def load(q):
        def do(w, p):
            for t in range(2):
                pltpu.make_async_copy(term(w, t, p, c), own.at[q % HELD, t], sem_load.at[0, t, q % 2]).start()
        of_weight(q, do)
        for t in range(2):
            wait(theirs.at[q, t], sem_swap_r.at[q, t])
            pltpu.make_async_copy(theirs.at[q, t], par.at[q % HELD, t], sem_load.at[1, t, q % 2]).start()

    def add(dst, *srcs):
        for k in range(COLS // 128):
            cut = (slice(None), slice(128 * k, 128 * k + 128))
            value = srcs[0][cut].astype(F32)
            for src in srcs[1:]:
                value = value + src[cut].astype(F32)
            dst[cut] = value.astype(dst.dtype)

    def both(q, t, i, j):
        a, b = at(t, i, j)
        return own.at[q % HELD, t, a, b], par.at[q % HELD, t, a, b]

    def freed(buf, sem, q):
        @pl.when(q >= SENT)
        def _():
            wait(buf, sem)

    def first(q, t, d):
        z, r = q % SENT, q % SLOTS
        return send(s1.at[z, t, d], r1.at[r, t, d], sem_s1.at[z, t, d], sem_r1.at[r, t, d], dev_i(t, (1, 3)[d]))

    def second(q, t, d, h):
        z, r = q % SENT, q % SLOTS
        return send(s2.at[z, t, d, h], r2.at[r, t, d, h], sem_s2.at[z, t, d, h], sem_r2.at[r, t, d, h], dev_i(t, (1, 3)[d]))

    def stage0(q):
        z = q % SENT
        for t in range(2):
            wait(own.at[q % HELD, t], sem_load.at[0, t, q % 2])
            wait(par.at[q % HELD, t], sem_load.at[1, t, q % 2])
        for t in range(2):
            i = place[t][0]
            for d in range(2):
                freed(s1.at[z, t, d], sem_s1.at[z, t, d], q)
                for b in range(2):
                    add(s1.at[z, t, d, b], *both(q, t, i + 2, 2 * d + b))
            for d in range(2):
                first(q, t, d).start()
        for t in range(2):
            i = place[t][0]
            for d in range(2):
                freed(s2.at[z, t, d, 1 - d], sem_s2.at[z, t, d, 1 - d], q)
                for b in range(2):
                    add(s2.at[z, t, d, 1 - d, b], *both(q, t, i + (1, 3)[d], 2 * (1 - d) + b))
            for d in range(2):
                second(q, t, d, 1 - d).start()

    def stage1(q):
        z, r = q % SENT, q % SLOTS
        for t in range(2):
            i = place[t][0]
            for d in range(2):
                freed(s2.at[z, t, d, d], sem_s2.at[z, t, d, d], q)
                wait(r1.at[r, t, d], sem_r1.at[r, t, d])
                for b in range(2):
                    add(s2.at[z, t, d, d, b], r1.at[r, t, d, b], *both(q, t, i + (1, 3)[d], 2 * d + b))
            for d in range(2):
                second(q, t, d, d).start()

    def cell(q, t, j):
        r, j = q % SLOTS, j % SIDE
        return (r2.at[r, t, 0, j // 2, j % 2], r2.at[r, t, 1, j // 2, j % 2], *both(q, t, place[t][0], j))

    def side(q):
        return 1 + 2 * (q % 2)

    def far(q, t):
        z, r = q % SENT, q % SLOTS
        return send(t1.at[z, t], u1.at[r, t], sem_t1.at[z, t], sem_u1.at[r, t], dev_j(t, side(q)))

    def near(q, t, e):
        z, r = q % SENT, q % SLOTS
        to = (side(q), SIDE - side(q))[e]
        return send(t2.at[z, t, e], u2.at[r, t, e], sem_t2.at[z, t, e], sem_u2.at[r, t, e], dev_j(t, to))

    def stage2(q):
        z, r = q % SENT, q % SLOTS
        for t in range(2):
            j = place[t][1]
            for d in range(2):
                for h in range(2):
                    wait(r2.at[r, t, d, h], sem_r2.at[r, t, d, h])
            freed(t1.at[z, t], sem_t1.at[z, t], q)
            freed(t2.at[z, t, 1], sem_t2.at[z, t, 1], q)
            add(t1.at[z, t], *cell(q, t, j + 2))
            add(t2.at[z, t, 1], *cell(q, t, j + SIDE - side(q)))
            far(q, t).start()
            near(q, t, 1).start()

    def stage3(q):
        z, r = q % SENT, q % SLOTS
        for t in range(2):
            freed(t2.at[z, t, 0], sem_t2.at[z, t, 0], q)
            wait(u1.at[r, t], sem_u1.at[r, t])
            add(t2.at[z, t, 0], u1.at[r, t], *cell(q, t, place[t][1] + side(q)))
            near(q, t, 0).start()

    def stage4(q):
        r = q % SLOTS
        for t in range(2):
            for e in range(2):
                wait(u2.at[r, t, e], sem_u2.at[r, t, e])
            add(total.at[q, t], u2.at[r, t, 0], u2.at[r, t, 1], *cell(q, t, place[t][1]))

    def adamw(dst, w, m, v, g):
        w, g = w.astype(F32), g.astype(F32)
        m = 0.9 * m + 0.1 * g
        v = 0.95 * v + 0.05 * g * g
        step = m * lax.rsqrt(v + 1e-8) + 0.1 * w
        dst[...] = (w - 0.02 * step).astype(BF16)

    third, mid = pieces // 2, 24
    top, cut = pieces * ROWS // 2 - third * ROWS, 16

    def parts(core):
        return [((third + 1) * core + k, 0, pl.multiple_of(mid * core + ROWS * k, 8), ROWS) for k in range(third)] + [
            (third, pl.multiple_of(cut * core, 16), pl.multiple_of(third * ROWS * (1 - core), 8), mid)]

    def loads_d():
        copies = [pltpu.make_async_copy(md, mbd, sem_m.at[0]), pltpu.make_async_copy(vd, vbd, sem_m.at[1])]
        rows = pl.ds(pl.multiple_of((third + 1) * ROWS * c, 8), third * ROWS)
        for t in range(2):
            copies.append(pltpu.make_async_copy(wd.at[t, x, y, rows], wb3.at[t], sem_m.at[2 + t]))
            rest = pl.ds(pl.multiple_of(third * ROWS + cut * c, 8), mid)
            copies.append(pltpu.make_async_copy(wd.at[t, x, y, rest], wbm.at[t], sem_m.at[4 + t]))
        return copies

    def swap_d(step):
        copies = []
        for t in range(2):
            if step == 0:
                three = (total.at[pl.ds((third + 1) * other, third), t], got3.at[t])
                rest = (total.at[third, t, pl.ds(pl.multiple_of(cut * other, 16), mid)], gotm.at[t])
            else:
                three = (put3.at[other, t], new.at[pl.ds((third + 1) * c, third), t])
                rest = (putm.at[other, t], newm.at[t])
            copies.append(send(*three, sem_xs.at[step, t, 0], sem_xr.at[step, t, 0], partner))
            copies.append(send(*rest, sem_xs.at[step, t, 1], sem_xr.at[step, t, 1], partner))
        return copies

    def sums_d():
        copies = []
        for t in range(2):
            for k, (piece, r, row, size) in enumerate(parts(c)):
                for h, src in enumerate((total.at[piece, t, pl.ds(r, size)], got3.at[t, k] if k < third else gotm.at[t])):
                    cols = pl.ds(pl.multiple_of((c, other)[h] * COLS, 128), COLS)
                    copies.append(pltpu.make_async_copy(src, sum_d.at[t, pl.ds(row, size), cols], sem_out.at[t, h, k]))
        return copies

    def step_d():
        for t in range(2):
            for k, (piece, r, row, size) in enumerate(parts(c)):
                for h in range(2):
                    g = (total.at[piece, t, pl.ds(r, size)], got3.at[t, k] if k < third else gotm.at[t])[h]
                    half = (c, other)[h]
                    dst = put3.at[half, t, k] if k < third else putm.at[half, t]
                    for b in range(COLS // 128):
                        lane = pl.ds(pl.multiple_of(half * COLS + 128 * b, 128), 128)
                        here = slice(128 * b, 128 * b + 128)
                        rows = pl.ds(row, size)
                        w = wb3[t, ROWS * k:ROWS * k + ROWS, lane] if k < third else wbm[t, :, lane]
                        adamw(dst.at[:, here], w, mbd[t, rows, lane], vbd[t, rows, lane], g[:, here])

    def merge_d():
        for t in range(2):
            for k in range(third):
                new[(third + 1) * c + k, t] = put3[c, t, k]
            a, b = putm[c, t], newm[t]
            low, high = jnp.where(c == 0, a, b), jnp.where(c == 0, b, a)
            line = lax.broadcasted_iota(jnp.int32, (mid - cut, COLS), 0)
            new[third, t, 0:cut] = low[0:cut]
            new[third, t, cut:mid] = jnp.where(line < top - cut, low[cut:mid].astype(F32), high[0:mid - cut].astype(F32)).astype(BF16)
            new[third, t, mid:ROWS] = high[mid - cut:mid]

    def loads_g(w):
        m, v, weight = ((mg, vg, wg), (mu, vu, wu))[w - 1]
        return [pltpu.make_async_copy(m, mbg, sem_m.at[6]), pltpu.make_async_copy(v, vbg, sem_m.at[7]), pltpu.make_async_copy(weight.at[:, x, y, c], wbg, sem_m.at[8])]

    def sums_g(w):
        out = (sum_g, sum_u)[w - 1]
        return [pltpu.make_async_copy(total.at[w * pieces + p], out.at[:, :, COLS * p:COLS * p + COLS], sem_out.at[p % 2, w - 1, p // 2]) for p in range(pieces)]

    def step_g(w):
        for t in range(2):
            for p in range(pieces):
                for b in range(COLS // 128):
                    here, lane = slice(128 * b, 128 * b + 128), slice(COLS * p + 128 * b, COLS * p + 128 * b + 128)
                    adamw(new.at[w * pieces + p, t, :, here], wbg[t, :, lane], mbg[t, :, lane], vbg[t, :, lane], total[w * pieces + p, t, :, here])

    def block(q, t, i, j):
        a, b = at(t, i, j)
        return whole.at[q, t, c, a, b]

    def line(q, t, i, h=None):
        some = slice(None) if h is None else pl.ds(2 * h, 2)
        return whole.at[q, t, c, i % SIDE, some] if t == 0 else whole.at[q, t, c, some, i % SIDE]

    def across(q, t, i):
        send(line(q, t, i), line(q, t, i), sem_os.at[t], sem_or.at[t], partner).start()

    def gather0(q):
        for t in range(2):
            i, j = place[t]
            for d in range(2):
                send(new.at[q, t], block(q, t, i, j), sem_gs.at[t, d], sem_gr.at[q, t, d], dev_j(t, (1, 3)[d])).start()
            pltpu.make_async_copy(new.at[q, t], block(q, t, i, j), sem_own.at[t, q % 4]).start()

    def gather1(q):
        for t in range(2):
            i, j = place[t]
            wait(new.at[q, t], sem_gr.at[q, t, 0])
            wait(new.at[q, t], sem_gr.at[q, t, 1])
            src = block(q, t, i, j + SIDE - side(q))
            send(src, src, sem_gs.at[t, 2], sem_gr.at[q, t, 2], dev_j(t, side(q))).start()
            wait(new.at[q, t], sem_own.at[t, q % 4])

    def gather2(q):
        for t in range(2):
            i = place[t][0]
            wait(new.at[q, t], sem_gr.at[q, t, 2])
            for d in range(2):
                send(line(q, t, i), line(q, t, i), sem_gs.at[t, 3 + d], sem_gr.at[q, t, 3 + d], dev_i(t, (1, 3)[d])).start()
            across(q, t, i)

    def gather3(q):
        for t in range(2):
            i = place[t][0]
            for d in range(2):
                there = i + (3, 1)[d]
                wait(line(q, t, there), sem_gr.at[q, t, 3 + d])
                send(line(q, t, there, d), line(q, t, there, d), sem_gs.at[t, 5 + d], sem_gr.at[q, t, 5 + d], dev_i(t, (1, 3)[d])).start()
            for d in range(2):
                across(q, t, i + (3, 1)[d])

    def gather4(q):
        for t in range(2):
            i = place[t][0]
            for d in range(2):
                wait(line(q, t, i + 2, d), sem_gr.at[q, t, 5 + d])
            across(q, t, i + 2)

    def when(q, do):
        @pl.when(jnp.logical_and(q >= 0, q < count))
        def _():
            do(q)

    def on(tick, t, do):
        @pl.when(t == tick)
        def _():
            do()

    barrier = pltpu.get_barrier_semaphore()
    peers = [dev(x + 1, y, c), dev(x + 3, y, c), dev(x, y + 1, c), dev(x, y + 3, c), partner]
    for peer in peers:
        pl.semaphore_signal(barrier, inc=1, device_id={"dp": peer}, device_id_type=MESH)
    pl.semaphore_wait(barrier, len(peers))

    for q in range(AHEAD):
        swap(q)
    load(0)
    for copy in loads_d() + loads_g(1):
        copy.start()

    ends = [w * pieces + pieces - 1 + LAG[4] for w in range(WEIGHTS)]
    gathers = ends[0] + 2
    stages = (stage0, stage1, stage2, stage3, stage4)
    rounds = (gather0, gather1, gather2, gather3, gather4)

    def start(copies):
        for copy in copies:
            copy.start()

    def finish(copies):
        for copy in copies:
            copy.wait()

    def d_begin():
        start(swap_d(0))

    def d_step():
        finish(loads_d())
        finish(swap_d(0))
        step_d()
        start(swap_d(1))
        start(sums_d())

    def d_end():
        finish(swap_d(1))
        merge_d()
        finish(sums_d())

    def g_step(w):
        finish(loads_g(w))
        step_g(w)
        if w + 1 < WEIGHTS:
            start(loads_g(w + 1))
        start(sums_g(w))

    def tick(t, _):
        when(t + AHEAD, swap)
        when(t + 1, load)
        for k in range(4, 0, -1):
            when(t - gathers - k, rounds[k])
        for k in range(4, -1, -1):
            when(t - LAG[k], stages[k])
        on(ends[0], t, d_begin)
        on(ends[0] + 1, t, d_step)
        on(ends[0] + 2, t, d_end)
        for w in range(1, WEIGHTS):
            on(ends[w], t, functools.partial(g_step, w))
            on(ends[w] + 1, t, lambda w=w: finish(sums_g(w)))
        when(t - gathers, gather0)
        return 0

    lax.fori_loop(0, count + gathers + 4, tick, 0)

    for z in range(SENT):
        for t in range(2):
            for d in range(2):
                wait(s1.at[z, t, d], sem_s1.at[z, t, d])
                wait(t2.at[z, t, d], sem_t2.at[z, t, d])
                for h in range(2):
                    wait(s2.at[z, t, d, h], sem_s2.at[z, t, d, h])
            wait(t1.at[z, t], sem_t1.at[z, t])
    for t in range(2):
        wait(theirs.at[:, t], sem_swap_s.at[t])
        for k in range(3):
            wait(new.at[:, t], sem_gs.at[t, k])
        for d in range(2):
            wait(whole.at[:, t, c, 0], sem_gs.at[t, 3 + d])
            wait(whole.at[:, t, c, 0, 0:2], sem_gs.at[t, 5 + d])
        wait(whole.at[:, t, c], sem_os.at[t])
        wait(whole.at[:, t, other], sem_or.at[t])


def put(pieces, slots, whole, out_d, out_g, out_u, buf, sem_in, sem_out):
    steps = [(w, t, x) for w in range(WEIGHTS) for t in range(2) for x in range(SIDE)]

    def load(s):
        w, t, x = steps[s]
        return pltpu.make_async_copy(whole.at[w * pieces:w * pieces + pieces, t, :, x], buf.at[s % slots], sem_in.at[s % slots])

    def stores(s):
        w, t, x = steps[s]
        copies = []
        for p in range(pieces):
            for c in range(CORES):
                if w == 0:
                    dst = out_d.at[t, x, :, ROWS * p:ROWS * p + ROWS, COLS * c:COLS * c + COLS]
                else:
                    dst = (out_g, out_u)[w - 1].at[t, x, :, c, :, COLS * p:COLS * p + COLS]
                copies.append(pltpu.make_async_copy(buf.at[s % slots, p, c], dst, sem_out.at[s % slots, p, c]))
        return copies

    ahead = slots // 2
    for s in range(ahead):
        load(s).start()
    for s in range(len(steps)):
        if s + ahead < len(steps):
            if s + ahead >= slots:
                for copy in stores(s + ahead - slots):
                    copy.wait()
            load(s + ahead).start()
        load(s).wait()
        for copy in stores(s):
            copy.start()
    for s in range(max(0, len(steps) - slots), len(steps)):
        for copy in stores(s):
            copy.wait()


def solution(mesh):
    devices = mesh.shape["dp"]
    assert devices == CORES * SIDE * SIDE

    def step(*arrays):
        (gg, gu, gd), (wg, wu, wd), (mg, mu, md), (vg, vu, vd) = (arrays[i : i + 3] for i in (0, 3, 6, 9))
        layers, rows, wide = wg.shape
        tall, narrow = wd.shape[1:]
        pieces = wide // COLS
        chip = tall // (SIDE * SIDE)
        assert layers == 2 and rows == devices * ROWS and narrow == CORES * COLS and chip == pieces * ROWS
        c = lax.axis_index("dp") % CORES
        window = pieces // 2 * ROWS + 24
        extra = window - chip // 2

        def shifted(a):
            return lax.dynamic_update_slice_in_dim(jnp.zeros((layers, window, narrow), F32), a, c * extra, 1)

        split_g = (layers, SIDE, SIDE, CORES, ROWS, wide)
        split_d = (layers, SIDE, SIDE, chip, narrow)
        block = (ROWS, COLS)
        count = WEIGHTS * pieces
        hbm = pl.BlockSpec(memory_space=pltpu.HBM)
        dma = pltpu.SemaphoreType.DMA
        third, mid = pieces // 2, 24
        whole, sum_d, sum_g, sum_u, _ = pl.pallas_call(
            functools.partial(fused, pieces),
            out_shape=(
                jax.ShapeDtypeStruct((count, 2, CORES, SIDE, SIDE, *block), BF16),
                jax.ShapeDtypeStruct((layers, window, narrow), BF16),
                jax.ShapeDtypeStruct((layers, ROWS, wide), BF16),
                jax.ShapeDtypeStruct((layers, ROWS, wide), BF16),
                jax.ShapeDtypeStruct((count, 2, SIDE, SIDE, *block), BF16),
            ),
            in_specs=[hbm] * 12,
            out_specs=[hbm] * 5,
            scratch_shapes=[
                pltpu.VMEM((HELD, 2, SIDE, SIDE, *block), BF16),
                pltpu.VMEM((HELD, 2, SIDE, SIDE, *block), BF16),
                pltpu.VMEM((SLOTS, 2, 2, 2, *block), BF16),
                pltpu.VMEM((SLOTS, 2, 2, 2, 2, *block), BF16),
                pltpu.VMEM((SLOTS, 2, *block), BF16),
                pltpu.VMEM((SLOTS, 2, 2, *block), BF16),
                pltpu.VMEM((SENT, 2, 2, 2, *block), BF16),
                pltpu.VMEM((SENT, 2, 2, 2, 2, *block), BF16),
                pltpu.VMEM((SENT, 2, *block), BF16),
                pltpu.VMEM((SENT, 2, 2, *block), BF16),
                pltpu.VMEM((count, 2, *block), BF16),
                pltpu.VMEM((count, 2, *block), BF16),
                pltpu.VMEM((2, third, *block), BF16),
                pltpu.VMEM((2, mid, COLS), BF16),
                pltpu.VMEM((CORES, 2, third, *block), BF16),
                pltpu.VMEM((CORES, 2, mid, COLS), BF16),
                pltpu.VMEM((2, mid, COLS), BF16),
                pltpu.VMEM((layers, window, narrow), F32),
                pltpu.VMEM((layers, window, narrow), F32),
                pltpu.VMEM((layers, third * ROWS, narrow), BF16),
                pltpu.VMEM((layers, mid, narrow), BF16),
                pltpu.VMEM((layers, ROWS, wide), F32),
                pltpu.VMEM((layers, ROWS, wide), F32),
                pltpu.VMEM((layers, ROWS, wide), BF16),
                dma((2, 2, 2)),
                dma((2,)),
                dma((count, 2)),
                dma((SLOTS, 2, 2)),
                dma((SLOTS, 2, 2, 2)),
                dma((SLOTS, 2)),
                dma((SLOTS, 2, 2)),
                dma((SENT, 2, 2)),
                dma((SENT, 2, 2, 2)),
                dma((SENT, 2)),
                dma((SENT, 2, 2)),
                dma((9,)),
                dma((2, 2, 4)),
                dma((2, 2, 2)),
                dma((2, 2, 2)),
                dma((2, 4)),
                dma((2, 7)),
                dma((count, 2, 7)),
                dma((2,)),
                dma((2,)),
            ],
            name="fused",
            compiler_params=pltpu.CompilerParams(collective_id=0, has_side_effects=True, vmem_limit_bytes=62 * 2**20),
        )(
            gd.reshape(split_d), gg.reshape(split_g), gu.reshape(split_g), wd.reshape(split_d), wg.reshape(split_g), wu.reshape(split_g),
            shifted(md), shifted(vd), mg, vg, mu, vu,
        )
        slots = 12
        new_d, new_g, new_u = pl.pallas_call(
            functools.partial(put, pieces, slots),
            out_shape=tuple(jax.ShapeDtypeStruct(s, BF16) for s in (split_d, split_g, split_g)),
            in_specs=[hbm],
            out_specs=[hbm] * 3,
            scratch_shapes=[pltpu.VMEM((slots, pieces, CORES, SIDE, *block), BF16), dma((slots,)), dma((slots, pieces, CORES))],
            name="put",
            compiler_params=pltpu.CompilerParams(vmem_limit_bytes=62 * 2**20),
        )(whole)
        g = (sum_g, sum_u, lax.dynamic_slice_in_dim(sum_d, c * extra, chip // 2, 1))
        g = [one.astype(F32) for one in g]
        m = [0.9 * a + 0.1 * b for a, b in zip((mg, mu, md), g)]
        v = [0.95 * a + 0.05 * b * b for a, b in zip((vg, vu, vd), g)]
        return (new_g.reshape(wg.shape), new_u.reshape(wu.shape), new_d.reshape(wd.shape), *m, *v)

    all_of, cut = P(None, None, None), P(None, "dp", None)
    return jax.shard_map(
        step,
        mesh=mesh,
        in_specs=(P(("rep", "dp"), None, None, None),) * 3 + (all_of,) * 3 + (cut,) * 6,
        out_specs=(P("rep", None, None),) * 3 + (P("rep", "dp", None),) * 6,
        check_vma=False,
    )
```

```python
import functools
import math

import jax
import jax.numpy as jnp
from jax import lax
from jax.experimental import pallas as pl
from jax.experimental.pallas import tpu as pltpu
from jax.sharding import PartitionSpec as P

MESH = pl.DeviceIdType.MESH
F32, BF16 = jnp.float32, jnp.bfloat16
CORES, SIDE = 2, 4
WEIGHTS = 3
ROWS, COLS = 40, 640
LAG = (0, 1, 2, 3, 4)
ROUND = (0, 2, 4, 6, 8, 9)
SLOTS = LAG[4] + LAG[2] + 2
HELD = LAG[4] + 2
SENT = 3
AHEAD = 3
FROM, TO = 6, 20


def fused(pieces, *refs):
    (gd, gg, gu, wd, wg, wu, md, vd, mg, vg, mu, vu, whole, kept, theirs, mbd, vbd, mbg, vbg, mbu, vbu,
     total, new, got3, gotm, put3, putm, newm, wb3, wbm, wbg,
     sem_load, sem_first, sem_swap_s, sem_swap_r, sem_r1, sem_r2, sem_u1, sem_u2, sem_s1, sem_s2, sem_t1, sem_t2,
     sem_m, sem_xs, sem_xr, sem_own, sem_gs, sem_gr, sem_os, sem_or, sem_kept) = refs
    count = WEIGHTS * pieces
    me = lax.axis_index("dp")
    x, y, c = me // (CORES * SIDE), (me // CORES) % SIDE, me % CORES
    other = 1 - c

    def dev(x, y, c):
        return ((x % SIDE) * SIDE + y % SIDE) * CORES + c

    partner = dev(x, y, other)
    place = ((x, y), (y, x))

    def dev_i(t, d):
        return dev(x + d, y, c) if t == 0 else dev(x, y + d, c)

    def dev_j(t, d):
        return dev_i(1 - t, d)

    def at(t, i, j):
        return (i % SIDE, j % SIDE) if t == 0 else (j % SIDE, i % SIDE)

    def send(src, dst, ssem, rsem, to):
        return pltpu.make_async_remote_copy(src_ref=src, dst_ref=dst, send_sem=ssem, recv_sem=rsem, device_id={"dp": to}, device_id_type=MESH)

    def wait(ref, sem):
        pltpu.make_async_copy(ref, ref, sem).wait()

    def own(q, t):
        return kept.at[q % HELD, t, 0]

    def par(q, t):
        return kept.at[q % HELD, t, 1]

    def r1(q, t, d):
        r = q % SLOTS
        return kept.at[HELD, t, d, r // 2, pl.ds(r % 2 * 2, 2)]

    def r2(q, t, d, h):
        r = q % SLOTS
        return kept.at[HELD + 1 + h, t, d, r // 2, pl.ds(r % 2 * 2, 2)]

    def u1(q, t):
        r = q % SLOTS
        return kept.at[HELD + 3, t, 0, 2 + r // SIDE, r % SIDE]

    def u2(q, t, e):
        r = q % SLOTS
        return kept.at[HELD + 3, t, e, r // SIDE, r % SIDE]

    def s1(q, t, d):
        return kept.at[HELD + 4, t, d, q % SENT, pl.ds(0, 2)]

    def s2(q, t, d, h):
        return kept.at[HELD + 5, t, d, q % SENT, pl.ds(2 * h, 2)]

    def t1(q, t):
        return kept.at[HELD + 4, t, 0, q % SENT, 2]

    def t2(q, t, e):
        return kept.at[HELD + 4, t, e, q % SENT, 3]

    def of_weight(q, do):
        for w in range(WEIGHTS):
            @pl.when(q // pieces == w)
            def _(w=w):
                do(w, q % pieces)

    def term(w, t, p, core):
        if w == 0:
            return gd.at[t, :, :, pl.ds(pl.multiple_of(p * ROWS, 8), ROWS), pl.ds(pl.multiple_of(core * COLS, 128), COLS)]
        return (gg, gu)[w - 1].at[t, :, :, core, :, pl.ds(pl.multiple_of(p * COLS, 128), COLS)]

    def swap(q):
        def do(w, p):
            for t in range(2):
                send(term(w, t, p, other), theirs.at[q, t], sem_swap_s.at[t], sem_swap_r.at[q, t], partner).start()
        of_weight(q, do)

    def load_own(q):
        def do(w, p):
            for t in range(2):
                pltpu.make_async_copy(term(w, t, p, c), own(q, t), sem_load.at[0, t, q % 2]).start()
        of_weight(q, do)

    def load(q):
        load_own(q)
        for t in range(2):
            wait(theirs.at[q, t], sem_swap_r.at[q, t])
            pltpu.make_async_copy(theirs.at[q, t], par(q, t), sem_load.at[1, t, q % 2]).start()

    def add(dst, *srcs):
        for k in range(COLS // 128):
            cut = (slice(None), slice(128 * k, 128 * k + 128))
            value = srcs[0][cut].astype(F32)
            for src in srcs[1:]:
                value = value + src[cut].astype(F32)
            dst[cut] = value.astype(dst.dtype)

    def both(q, t, i, j):
        a, b = at(t, i, j)
        return own(q, t).at[a, b], par(q, t).at[a, b]

    def freed(buf, sem, q):
        @pl.when(q >= SENT)
        def _():
            wait(buf, sem)

    def first(q, t, d):
        return send(s1(q, t, d), r1(q, t, d), sem_s1.at[q % SENT, t, d], sem_r1.at[q % SLOTS, t, d], dev_i(t, (1, 3)[d]))

    def second(q, t, d, h):
        return send(s2(q, t, d, h), r2(q, t, d, h), sem_s2.at[q % SENT, t, d, h], sem_r2.at[q % SLOTS, t, d, h], dev_i(t, (1, 3)[d]))

    def far_chunk(q, t):
        for d in range(2):
            for b in range(2):
                add(s1(q, t, d).at[b], *both(q, t, place[t][0] + 2, 2 * d + b))
        for d in range(2):
            first(q, t, d).start()

    def near_chunks(q, t):
        for d in range(2):
            for b in range(2):
                add(s2(q, t, d, 1 - d).at[b], *both(q, t, place[t][0] + (1, 3)[d], 2 * (1 - d) + b))
        for d in range(2):
            second(q, t, d, 1 - d).start()

    def chunk(t, k):
        def of(ref):
            i = (place[t][0] + (2, 1, 3, 0)[k]) % SIDE
            return ref.at[i] if t == 0 else ref.at[:, i]
        return send(of(term(0, t, 0, other)), of(par(0, t)), sem_first.at[0, t, k], sem_first.at[1, t, k], partner)

    def stage0_first():
        for t in range(2):
            wait(own(0, t), sem_load.at[0, t, 0])
            chunk(t, 0).wait_recv()
            far_chunk(0, t)
        for t in range(2):
            for k in range(1, 3):
                chunk(t, k).wait_recv()
            near_chunks(0, t)
        for t in range(2):
            chunk(t, 3).wait_recv()
            for k in range(4):
                chunk(t, k).wait_send()

    def stage0(q):
        for t in range(2):
            wait(own(q, t), sem_load.at[0, t, q % 2])
            wait(par(q, t), sem_load.at[1, t, q % 2])
        for t in range(2):
            for d in range(2):
                freed(s1(q, t, d), sem_s1.at[q % SENT, t, d], q)
            far_chunk(q, t)
        for t in range(2):
            for d in range(2):
                freed(s2(q, t, d, 1 - d), sem_s2.at[q % SENT, t, d, 1 - d], q)
            near_chunks(q, t)

    def stage1(q):
        for t in range(2):
            for d in range(2):
                freed(s2(q, t, d, d), sem_s2.at[q % SENT, t, d, d], q)
                wait(r1(q, t, d), sem_r1.at[q % SLOTS, t, d])
                for b in range(2):
                    add(s2(q, t, d, d).at[b], r1(q, t, d).at[b], *both(q, t, place[t][0] + (1, 3)[d], 2 * d + b))
            for d in range(2):
                second(q, t, d, d).start()

    def cell(q, t, j):
        j = j % SIDE
        came = [kept.at[HELD + 1 + j // 2, t, d, q % SLOTS // 2, q % SLOTS % 2 * 2 + j % 2] for d in range(2)]
        return (*came, *both(q, t, place[t][0], j))

    def side(q):
        return 1 + 2 * (q % 2)

    def far(q, t):
        return send(t1(q, t), u1(q, t), sem_t1.at[q % SENT, t], sem_u1.at[q % SLOTS, t], dev_j(t, side(q)))

    def near(q, t, e):
        to = (side(q), SIDE - side(q))[e]
        return send(t2(q, t, e), u2(q, t, e), sem_t2.at[q % SENT, t, e], sem_u2.at[q % SLOTS, t, e], dev_j(t, to))

    def stage2(q):
        for t in range(2):
            j = place[t][1]
            for d in range(2):
                for h in range(2):
                    wait(r2(q, t, d, h), sem_r2.at[q % SLOTS, t, d, h])
            freed(t1(q, t), sem_t1.at[q % SENT, t], q)
            freed(t2(q, t, 1), sem_t2.at[q % SENT, t, 1], q)
            add(t1(q, t), *cell(q, t, j + 2))
            add(t2(q, t, 1), *cell(q, t, j + SIDE - side(q)))
            far(q, t).start()
            near(q, t, 1).start()

    def stage3(q):
        for t in range(2):
            freed(t2(q, t, 0), sem_t2.at[q % SENT, t, 0], q)
            wait(u1(q, t), sem_u1.at[q % SLOTS, t])
            add(t2(q, t, 0), u1(q, t), *cell(q, t, place[t][1] + side(q)))
            near(q, t, 0).start()

    def stage4(q):
        for t in range(2):
            for e in range(2):
                wait(u2(q, t, e), sem_u2.at[q % SLOTS, t, e])
            add(total.at[q, t], u2(q, t, 0), u2(q, t, 1), *cell(q, t, place[t][1]))

    def adamw(dst, w, m, v, g):
        w, g = w.astype(F32), g.astype(F32)
        m = 0.9 * m + 0.1 * g
        v = 0.95 * v + 0.05 * g * g
        step = m * lax.rsqrt(v + 1e-8) + 0.1 * w
        dst[...] = (w - 0.02 * step).astype(BF16)
        return m, v

    third, mid = pieces // 2, 24
    top, cut = pieces * ROWS // 2 - third * ROWS, 16

    def parts(core):
        return [((third + 1) * core + k, 0, pl.multiple_of(mid * core + ROWS * k, 8), ROWS) for k in range(third)] + [
            (third, pl.multiple_of(cut * core, 16), pl.multiple_of(third * ROWS * (1 - core), 8), mid)]

    mine = pl.ds((mid + third * ROWS - md.shape[0]) * c, md.shape[0])

    def loads_d():
        copies = [pltpu.make_async_copy(md, mbd.at[mine], sem_m.at[0, 0]), pltpu.make_async_copy(vd, vbd.at[mine], sem_m.at[1, 0])]
        rows = pl.ds(pl.multiple_of((third + 1) * ROWS * c, 8), third * ROWS)
        for t in range(2):
            copies.append(pltpu.make_async_copy(wd.at[t, x, y, rows], wb3.at[t], sem_m.at[2 + t, 0]))
            rest = pl.ds(pl.multiple_of(third * ROWS + cut * c, 8), mid)
            copies.append(pltpu.make_async_copy(wd.at[t, x, y, rest], wbm.at[t], sem_m.at[4 + t, 0]))
        return copies

    def swap_d(step):
        copies = []
        for t in range(2):
            if step == 0:
                three = (total.at[pl.ds((third + 1) * other, third), t], got3.at[t])
                rest = (total.at[third, t, pl.ds(pl.multiple_of(cut * other, 16), mid)], gotm.at[t])
            else:
                three = (put3.at[other, t], new.at[pl.ds((third + 1) * c, third), t])
                rest = (putm.at[other, t], newm.at[t])
            copies.append(send(*three, sem_xs.at[step, t, 0], sem_xr.at[step, t, 0], partner))
            copies.append(send(*rest, sem_xs.at[step, t, 1], sem_xr.at[step, t, 1], partner))
        return copies

    def step_d():
        for t in range(2):
            for k, (piece, r, row, size) in enumerate(parts(c)):
                for h in range(2):
                    g = (total.at[piece, t, pl.ds(r, size)], got3.at[t, k] if k < third else gotm.at[t])[h]
                    half = (c, other)[h]
                    dst = put3.at[half, t, k] if k < third else putm.at[half, t]
                    for b in range(COLS // 128):
                        lane = pl.ds(pl.multiple_of(half * COLS + 128 * b, 128), 128)
                        here = slice(128 * b, 128 * b + 128)
                        rows = pl.ds(row, size)
                        w = wb3[t, ROWS * k:ROWS * k + ROWS, lane] if k < third else wbm[t, :, lane]
                        mbd[rows, t, lane], vbd[rows, t, lane] = adamw(dst.at[:, here], w, mbd[rows, t, lane], vbd[rows, t, lane], g[:, here])

    def merge_d():
        for t in range(2):
            for k in range(third):
                new[(third + 1) * c + k, t] = put3[c, t, k]
            a, b = putm[c, t], newm[t]
            low, high = jnp.where(c == 0, a, b), jnp.where(c == 0, b, a)
            line = lax.broadcasted_iota(jnp.int32, (mid - cut, COLS), 0)
            new[third, t, 0:cut] = low[0:cut]
            new[third, t, cut:mid] = jnp.where(line < top - cut, low[cut:mid].astype(F32), high[0:mid - cut].astype(F32)).astype(BF16)
            new[third, t, mid:ROWS] = high[mid - cut:mid]

    def loads_g(w):
        (m, v), (mb, vb) = (((mg, vg), (mbg, vbg)), ((mu, vu), (mbu, vbu)))[w - 1]
        return [pltpu.make_async_copy(m, mb, sem_m.at[6, w - 1]), pltpu.make_async_copy(v, vb, sem_m.at[7, w - 1])]

    def load_w(w):
        return pltpu.make_async_copy((wg, wu)[w - 1].at[:, x, y, c], wbg, sem_m.at[8, w - 1])

    def step_g(w):
        mb, vb = ((mbg, vbg), (mbu, vbu))[w - 1]
        for t in range(2):
            for p in range(pieces):
                for b in range(COLS // 128):
                    here, lane = slice(128 * b, 128 * b + 128), slice(COLS * p + 128 * b, COLS * p + 128 * b + 128)
                    mb[t, :, lane], vb[t, :, lane] = adamw(
                        new.at[w * pieces + p, t, :, here], wbg[t, :, lane], mb[t, :, lane], vb[t, :, lane], total[w * pieces + p, t, :, here])

    def block(q, t, i, j):
        a, b = at(t, i, j)
        return whole.at[q, t, c, a, b]

    def line(q, t, i, h=None):
        some = slice(None) if h is None else pl.ds(2 * h, 2)
        return whole.at[q, t, c, i % SIDE, some] if t == 0 else whole.at[q, t, c, some, i % SIDE]

    def across(q, t, i):
        send(line(q, t, i), line(q, t, i), sem_os.at[t], sem_or.at[q, t], partner).start()

    def gather0(q):
        for t in range(2):
            i, j = place[t]
            for d in range(2):
                send(new.at[q, t], block(q, t, i, j), sem_gs.at[t, d], sem_gr.at[q, t, d], dev_j(t, (1, 3)[d])).start()
            pltpu.make_async_copy(new.at[q, t], block(q, t, i, j), sem_own.at[t, q % 4]).start()

    def gather1(q):
        for t in range(2):
            i, j = place[t]
            wait(new.at[q, t], sem_gr.at[q, t, 0])
            wait(new.at[q, t], sem_gr.at[q, t, 1])
            src = block(q, t, i, j + SIDE - side(q))
            send(src, src, sem_gs.at[t, 2], sem_gr.at[q, t, 2], dev_j(t, side(q))).start()
            wait(new.at[q, t], sem_own.at[t, q % 4])

    def gather2(q):
        for t in range(2):
            i = place[t][0]
            wait(new.at[q, t], sem_gr.at[q, t, 2])
            for k in range(2):
                for d in range(2):
                    half = line(q, t, i, (d, 1 - d)[k])
                    send(half, half, sem_gs.at[t, 3 + 2 * k + d], sem_gr.at[q, t, 3 + 2 * k + d], dev_i(t, (1, 3)[d])).start()
            across(q, t, i)

    def gather3(q):
        for t in range(2):
            for d in range(2):
                half = line(q, t, place[t][0] + (3, 1)[d], d)
                wait(half, sem_gr.at[q, t, 3 + d])
                send(half, half, sem_gs.at[t, 7 + d], sem_gr.at[q, t, 7 + d], dev_i(t, (1, 3)[d])).start()
        for t in range(2):
            for d in range(2):
                there = place[t][0] + (3, 1)[d]
                wait(line(q, t, there, 1 - d), sem_gr.at[q, t, 5 + d])
                across(q, t, there)

    def gather4(q):
        for t in range(2):
            i = place[t][0]
            for d in range(2):
                wait(line(q, t, i + 2, d), sem_gr.at[q, t, 7 + d])
            across(q, t, i + 2)

    def keep(q):
        for t in range(2):
            wait(whole.at[q, t, other], sem_or.at[q, t])

        @pl.when(jnp.logical_and(q >= FROM, q < TO))
        def _():
            pltpu.make_async_copy(whole.at[q], kept.at[q - FROM], sem_kept).start()

    def when(q, do):
        @pl.when(jnp.logical_and(q >= 0, q < count))
        def _():
            do(q)

    def on(tick, t, do):
        @pl.when(t == tick)
        def _():
            do()

    load_own(0)
    barrier = pltpu.get_barrier_semaphore()
    peers = [dev(x + 1, y, c), dev(x + 3, y, c), dev(x, y + 1, c), dev(x, y + 3, c), partner]
    for peer in peers:
        pl.semaphore_signal(barrier, inc=1, device_id={"dp": peer}, device_id_type=MESH)
    pl.semaphore_wait(barrier, len(peers))
    for k in range(4):
        for t in range(2):
            chunk(t, k).start()
    for q in range(1, AHEAD):
        swap(q)
    for copy in loads_d() + loads_g(1) + loads_g(2) + [load_w(1)]:
        copy.start()
    stage0_first()

    ends = [w * pieces + pieces - 1 + LAG[4] for w in range(WEIGHTS)]
    gathers = ends[0] + 2
    stages = (stage0, stage1, stage2, stage3, stage4)
    rounds = (gather0, gather1, gather2, gather3, gather4, keep)
    assert FROM + gathers + ROUND[5] > ends[-1] + 1 and TO - FROM == kept.shape[0] and HELD + 6 <= TO - FROM

    def start(copies):
        for copy in copies:
            copy.start()

    def finish(copies):
        for copy in copies:
            copy.wait()

    def d_begin():
        start(swap_d(0))

    def d_step():
        finish(loads_d())
        finish(swap_d(0))
        step_d()
        start(swap_d(1))

    def d_end():
        finish(swap_d(1))
        merge_d()

    def g_step(w):
        finish(loads_g(w))
        load_w(w).wait()
        step_g(w)
        if w + 1 < WEIGHTS:
            load_w(w + 1).start()

    def sent():
        for z in range(SENT):
            for t in range(2):
                for d in range(2):
                    wait(s1(z, t, d), sem_s1.at[z, t, d])
                    wait(t2(z, t, d), sem_t2.at[z, t, d])
                    for h in range(2):
                        wait(s2(z, t, d, h), sem_s2.at[z, t, d, h])
                wait(t1(z, t), sem_t1.at[z, t])

    def tick(t, _):
        when(t + AHEAD, swap)
        when(t + 1, load)
        for k in range(5, 0, -1):
            when(t - gathers - ROUND[k], rounds[k])
        for k in range(4, 0, -1):
            when(t - LAG[k], stages[k])

        @pl.when(t > 0)
        def _():
            when(t, stage0)
        on(ends[0], t, d_begin)
        on(ends[0] + 1, t, d_step)
        on(ends[0] + 2, t, d_end)
        for w in range(1, WEIGHTS):
            on(ends[w], t, functools.partial(g_step, w))
        on(ends[-1] + 1, t, sent)
        when(t - gathers, gather0)
        return 0

    lax.fori_loop(0, count + gathers + ROUND[5], tick, 0)

    for t in range(2):
        wait(theirs.at[1:, t], sem_swap_s.at[t])
        for k in range(3):
            wait(new.at[:, t], sem_gs.at[t, k])
        for d in range(2):
            for k in range(3):
                wait(whole.at[:, t, c, 0, 0:2], sem_gs.at[t, 3 + 2 * k + d])
        wait(whole.at[:, t, c], sem_os.at[t])
    wait(kept, sem_kept)


def put(pieces, slots, whole, kept, mbd, vbd, mbg, vbg, mbu, vbu, out_d, out_g, out_u, md, vd, mg, vg, mu, vu, buf, sem_in, sem_out, sem_kept, sem_m):
    steps = [(q, t) for q in range(WEIGHTS * pieces) for t in range(2) if not FROM <= q < TO]
    rest = [(q, t) for q in range(FROM, TO) for t in range(2)]

    def dst(q, t, c):
        w, p = divmod(q, pieces)
        if w == 0:
            return out_d.at[t, :, :, ROWS * p:ROWS * p + ROWS, COLS * c:COLS * c + COLS]
        return (out_g, out_u)[w - 1].at[t, :, :, c, :, COLS * p:COLS * p + COLS]

    def load(s):
        q, t = steps[s]
        return pltpu.make_async_copy(whole.at[q, t], buf.at[s % slots], sem_in.at[s % slots])

    def stores(s):
        return [pltpu.make_async_copy(buf.at[s % slots, c], dst(*steps[s], c), sem_out.at[s % slots, c]) for c in range(CORES)]

    mine = pl.ds((mbd.shape[0] - md.shape[0]) * (lax.axis_index("dp") % CORES), md.shape[0])
    moments = [(mbd.at[mine], md), (vbd.at[mine], vd), (mbg, mg), (vbg, vg), (mbu, mu), (vbu, vu)]
    moments = [pltpu.make_async_copy(src, dst, sem_m.at[k]) for k, (src, dst) in enumerate(moments)]
    ahead = slots // 2
    for s in range(ahead):
        load(s).start()
    for copy in moments:
        copy.start()
    for s in range(len(steps)):
        for q, t in rest[len(rest) * s // len(steps):len(rest) * (s + 1) // len(steps)]:
            for c in range(CORES):
                pltpu.make_async_copy(kept.at[q - FROM, t, c], dst(q, t, c), sem_kept).start()
        if s + ahead < len(steps):
            if s + ahead >= slots:
                for copy in stores(s + ahead - slots):
                    copy.wait()
            load(s + ahead).start()
        load(s).wait()
        for copy in stores(s):
            copy.start()
    for s in range(max(0, len(steps) - slots), len(steps)):
        for copy in stores(s):
            copy.wait()
    pltpu.make_async_copy(kept, kept, sem_kept).wait()
    for copy in moments:
        copy.wait()


def solution(mesh):
    devices = mesh.shape["dp"]
    assert devices == CORES * SIDE * SIDE

    def step(*arrays):
        (gg, gu, gd), (wg, wu, wd), (mg, mu, md), (vg, vu, vd) = (arrays[i : i + 3] for i in (0, 3, 6, 9))
        layers, rows, wide = wg.shape
        tall, narrow = wd.shape[1:]
        pieces = wide // COLS
        chip = tall // (SIDE * SIDE)
        assert layers == 2 and rows == devices * ROWS and narrow == CORES * COLS and chip == pieces * ROWS
        split_g = (layers, SIDE, SIDE, CORES, ROWS, wide)
        split_d = (layers, SIDE, SIDE, chip, narrow)
        block = (ROWS, COLS)
        count = WEIGHTS * pieces
        hbm, vmem = pl.BlockSpec(memory_space=pltpu.HBM), pl.BlockSpec(memory_space=pltpu.VMEM)
        dma = pltpu.SemaphoreType.DMA
        third, mid = pieces // 2, 24
        window = third * ROWS + mid
        md, vd = (a.transpose(1, 0, 2) for a in (md, vd))
        whole, kept, _, *moments = pl.pallas_call(
            functools.partial(fused, pieces),
            out_shape=(
                jax.ShapeDtypeStruct((count, 2, CORES, SIDE, SIDE, *block), BF16),
                pltpu.VMEM((TO - FROM, 2, CORES, SIDE, SIDE, *block), BF16),
                jax.ShapeDtypeStruct((count, 2, SIDE, SIDE, *block), BF16),
                *(pltpu.VMEM((window, *md.shape[1:]), F32) for _ in range(2)),
                *(pltpu.VMEM(mg.shape, F32) for _ in range(4)),
            ),
            in_specs=[hbm] * 12,
            out_specs=[hbm, vmem, hbm] + [vmem] * 6,
            scratch_shapes=[
                pltpu.VMEM((count, 2, *block), BF16),
                pltpu.VMEM((count, 2, *block), BF16),
                pltpu.VMEM((2, third, *block), BF16),
                pltpu.VMEM((2, mid, COLS), BF16),
                pltpu.VMEM((CORES, 2, third, *block), BF16),
                pltpu.VMEM((CORES, 2, mid, COLS), BF16),
                pltpu.VMEM((2, mid, COLS), BF16),
                pltpu.VMEM((layers, third * ROWS, narrow), BF16),
                pltpu.VMEM((layers, mid, narrow), BF16),
                pltpu.VMEM((layers, ROWS, wide), BF16),
                dma((2, 2, 2)),
                dma((2, 2, 4)),
                dma((2,)),
                dma((count, 2)),
                dma((SLOTS, 2, 2)),
                dma((SLOTS, 2, 2, 2)),
                dma((SLOTS, 2)),
                dma((SLOTS, 2, 2)),
                dma((SENT, 2, 2)),
                dma((SENT, 2, 2, 2)),
                dma((SENT, 2)),
                dma((SENT, 2, 2)),
                dma((9, 2)),
                dma((2, 2, 2)),
                dma((2, 2, 2)),
                dma((2, 4)),
                dma((2, 9)),
                dma((count, 2, 9)),
                dma((2,)),
                dma((count, 2)),
                dma,
            ],
            name="fused",
            compiler_params=pltpu.CompilerParams(collective_id=0, has_side_effects=True, vmem_limit_bytes=10 * 2**20),
        )(
            gd.reshape(split_d), gg.reshape(split_g), gu.reshape(split_g), wd.reshape(split_d), wg.reshape(split_g), wu.reshape(split_g),
            md, vd, mg, vg, mu, vu,
        )
        slots = 6
        new_d, new_g, new_u, md, vd, mg, vg, mu, vu = pl.pallas_call(
            functools.partial(put, pieces, slots),
            out_shape=(*(jax.ShapeDtypeStruct(s, BF16) for s in (split_d, split_g, split_g)), *(jax.ShapeDtypeStruct(a.shape, F32) for a in (md, vd, mg, vg, mu, vu))),
            in_specs=[hbm] + [vmem] * 7,
            out_specs=[hbm] * 9,
            scratch_shapes=[pltpu.VMEM((slots, CORES, SIDE, SIDE, *block), BF16), dma((slots,)), dma((slots, CORES)), dma, dma((6,))],
            name="put",
            compiler_params=pltpu.CompilerParams(vmem_limit_bytes=10 * 2**20),
        )(whole, *(pltpu.with_memory_space_constraint(a, pltpu.VMEM) for a in (kept, *moments)))
        md, vd = (a.transpose(1, 0, 2) for a in (md, vd))
        return (new_g.reshape(wg.shape), new_u.reshape(wu.shape), new_d.reshape(wd.shape), mg, mu, md, vg, vu, vd)

    all_of, cut = P(None, None, None), P(None, "dp", None)
    return jax.shard_map(
        step,
        mesh=mesh,
        in_specs=(P(("rep", "dp"), None, None, None),) * 3 + (all_of,) * 3 + (cut,) * 6,
        out_specs=(P("rep", None, None),) * 3 + (P("rep", "dp", None),) * 6,
        check_vma=False,
    )
```

```python
import functools
import math

import jax
import jax.numpy as jnp
from jax import lax
from jax.experimental import pallas as pl
from jax.experimental.pallas import tpu as pltpu
from jax.sharding import PartitionSpec as P

MESH = pl.DeviceIdType.MESH
F32, BF16 = jnp.float32, jnp.bfloat16
CORES, SIDE = 2, 4
WEIGHTS = 3
ROWS, COLS = 40, 640
LAG = (0, 1, 2, 3, 4)
ROUND = (0, 2, 4, 6, 8, 9)
SLOTS = LAG[4] + LAG[2] + 2
HELD = LAG[4] + 2
SENT = 3
AHEAD = 3
DIRECT, PULLED = 14, 6
TURNS = 8


def fused(pieces, *refs):
    (gd, gg, gu, wd, wg, wu, md, vd, mg, vg, mu, vu, whole, kept, theirs, mbd, vbd, mbg, vbg, mbu, vbu,
     total_ref, new_ref, got3, gotm, put3, putm, newm, wb3, wbm, wbg,
     sem_load, sem_first, sem_swap_s, sem_swap_r, sem_r1, sem_r2, sem_u1, sem_u2, sem_s1, sem_s2, sem_t1, sem_t2,
     sem_m, sem_xs, sem_xr, sem_own, sem_gs, sem_gr, sem_os, sem_or, sem_kept, sem_free) = refs
    count = WEIGHTS * pieces
    me = lax.axis_index("dp")
    x, y, c = me // (CORES * SIDE), (me // CORES) % SIDE, me % CORES
    other = 1 - c

    def dev(x, y, c):
        return ((x % SIDE) * SIDE + y % SIDE) * CORES + c

    partner = dev(x, y, other)
    place = ((x, y), (y, x))

    def dev_i(t, d):
        return dev(x + d, y, c) if t == 0 else dev(x, y + d, c)

    def dev_j(t, d):
        return dev_i(1 - t, d)

    def at(t, i, j):
        return (i % SIDE, j % SIDE) if t == 0 else (j % SIDE, i % SIDE)

    def send(src, dst, ssem, rsem, to):
        return pltpu.make_async_remote_copy(src_ref=src, dst_ref=dst, send_sem=ssem, recv_sem=rsem, device_id={"dp": to}, device_id_type=MESH)

    def wait(ref, sem):
        pltpu.make_async_copy(ref, ref, sem).wait()

    def own(q, t):
        return kept.at[q % HELD, t, 0]

    def par(q, t):
        return kept.at[q % HELD, t, 1]

    def r1(q, t, d):
        r = q % SLOTS
        return kept.at[HELD, t, d, r // 2, pl.ds(r % 2 * 2, 2)]

    def r2(q, t, d, h):
        r = q % SLOTS
        return kept.at[HELD + 1 + h, t, d, r // 2, pl.ds(r % 2 * 2, 2)]

    def u1(q, t):
        r = q % SLOTS
        return kept.at[HELD + 3, t, 0, 2 + r // SIDE, r % SIDE]

    def u2(q, t, e):
        r = q % SLOTS
        return kept.at[HELD + 3, t, e, r // SIDE, r % SIDE]

    def s1(q, t, d):
        return kept.at[HELD + 4, t, d, q % SENT, pl.ds(0, 2)]

    def s2(q, t, d, h):
        return kept.at[HELD + 5, t, d, q % SENT, pl.ds(2 * h, 2)]

    def t1(q, t):
        return kept.at[HELD + 4, t, 0, q % SENT, 2]

    def t2(q, t, e):
        return kept.at[HELD + 4, t, e, q % SENT, 3]

    def total(q, t):
        return total_ref.at[q, t]

    def new(q, t):
        return new_ref.at[q, t]

    def of_weight(q, do):
        for w in range(WEIGHTS):
            @pl.when(q // pieces == w)
            def _(w=w):
                do(w, q % pieces)

    def term(w, t, p, core):
        if w == 0:
            return gd.at[t, :, :, pl.ds(pl.multiple_of(p * ROWS, 8), ROWS), pl.ds(pl.multiple_of(core * COLS, 128), COLS)]
        return (gg, gu)[w - 1].at[t, :, :, core, :, pl.ds(pl.multiple_of(p * COLS, 128), COLS)]

    def swap(q):
        def do(w, p):
            for t in range(2):
                send(term(w, t, p, other), theirs.at[q, t], sem_swap_s.at[t], sem_swap_r.at[q % TURNS, t], partner).start()
        of_weight(q, do)

    def load_own(q):
        def do(w, p):
            for t in range(2):
                pltpu.make_async_copy(term(w, t, p, c), own(q, t), sem_load.at[0, t, q % 2]).start()
        of_weight(q, do)

    def load(q):
        load_own(q)
        for t in range(2):
            wait(theirs.at[q, t], sem_swap_r.at[q % TURNS, t])
            pltpu.make_async_copy(theirs.at[q, t], par(q, t), sem_load.at[1, t, q % 2]).start()

    def add(dst, *srcs):
        for k in range(COLS // 128):
            cut = (slice(None), slice(128 * k, 128 * k + 128))
            value = srcs[0][cut].astype(F32)
            for src in srcs[1:]:
                value = value + src[cut].astype(F32)
            dst[cut] = value.astype(dst.dtype)

    def both(q, t, i, j):
        a, b = at(t, i, j)
        return own(q, t).at[a, b], par(q, t).at[a, b]

    def freed(buf, sem, q):
        @pl.when(q >= SENT)
        def _():
            wait(buf, sem)

    def first(q, t, d):
        return send(s1(q, t, d), r1(q, t, d), sem_s1.at[q % SENT, t, d], sem_r1.at[q % SLOTS, t, d], dev_i(t, (1, 3)[d]))

    def second(q, t, d, h):
        return send(s2(q, t, d, h), r2(q, t, d, h), sem_s2.at[q % SENT, t, d, h], sem_r2.at[q % SLOTS, t, d, h], dev_i(t, (1, 3)[d]))

    def far_chunk(q, t):
        for d in range(2):
            for b in range(2):
                add(s1(q, t, d).at[b], *both(q, t, place[t][0] + 2, 2 * d + b))
        for d in range(2):
            first(q, t, d).start()

    def near_chunks(q, t):
        for d in range(2):
            for b in range(2):
                add(s2(q, t, d, 1 - d).at[b], *both(q, t, place[t][0] + (1, 3)[d], 2 * (1 - d) + b))
        for d in range(2):
            second(q, t, d, 1 - d).start()

    def chunk(t, k):
        def of(ref):
            i = (place[t][0] + (2, 1, 3, 0)[k]) % SIDE
            return ref.at[i] if t == 0 else ref.at[:, i]
        return send(of(term(0, t, 0, other)), of(par(0, t)), sem_first.at[0, t, k], sem_first.at[1, t, k], partner)

    def stage0_first():
        for t in range(2):
            wait(own(0, t), sem_load.at[0, t, 0])
            chunk(t, 0).wait_recv()
            far_chunk(0, t)
        for t in range(2):
            for k in range(1, 3):
                chunk(t, k).wait_recv()
            near_chunks(0, t)

    def stage0_rest():
        for t in range(2):
            chunk(t, 3).wait_recv()
            for k in range(4):
                chunk(t, k).wait_send()

    def stage0(q):
        for t in range(2):
            wait(own(q, t), sem_load.at[0, t, q % 2])
            wait(par(q, t), sem_load.at[1, t, q % 2])
        for t in range(2):
            for d in range(2):
                freed(s1(q, t, d), sem_s1.at[q % SENT, t, d], q)
            far_chunk(q, t)
        for t in range(2):
            for d in range(2):
                freed(s2(q, t, d, 1 - d), sem_s2.at[q % SENT, t, d, 1 - d], q)
            near_chunks(q, t)

    def stage1(q):
        for t in range(2):
            for d in range(2):
                freed(s2(q, t, d, d), sem_s2.at[q % SENT, t, d, d], q)
                wait(r1(q, t, d), sem_r1.at[q % SLOTS, t, d])
                for b in range(2):
                    add(s2(q, t, d, d).at[b], r1(q, t, d).at[b], *both(q, t, place[t][0] + (1, 3)[d], 2 * d + b))
            for d in range(2):
                second(q, t, d, d).start()

    def cell(q, t, j):
        j = j % SIDE
        came = [kept.at[HELD + 1 + j // 2, t, d, q % SLOTS // 2, q % SLOTS % 2 * 2 + j % 2] for d in range(2)]
        return (*came, *both(q, t, place[t][0], j))

    def side(q):
        return 1 + 2 * (q % 2)

    def far(q, t):
        return send(t1(q, t), u1(q, t), sem_t1.at[q % SENT, t], sem_u1.at[q % SLOTS, t], dev_j(t, side(q)))

    def near(q, t, e):
        to = (side(q), SIDE - side(q))[e]
        return send(t2(q, t, e), u2(q, t, e), sem_t2.at[q % SENT, t, e], sem_u2.at[q % SLOTS, t, e], dev_j(t, to))

    def stage2(q):
        for t in range(2):
            j = place[t][1]
            for d in range(2):
                for h in range(2):
                    wait(r2(q, t, d, h), sem_r2.at[q % SLOTS, t, d, h])
            freed(t1(q, t), sem_t1.at[q % SENT, t], q)
            freed(t2(q, t, 1), sem_t2.at[q % SENT, t, 1], q)
            add(t1(q, t), *cell(q, t, j + 2))
            add(t2(q, t, 1), *cell(q, t, j + SIDE - side(q)))
            far(q, t).start()
            near(q, t, 1).start()

    def stage3(q):
        for t in range(2):
            freed(t2(q, t, 0), sem_t2.at[q % SENT, t, 0], q)
            wait(u1(q, t), sem_u1.at[q % SLOTS, t])
            add(t2(q, t, 0), u1(q, t), *cell(q, t, place[t][1] + side(q)))
            near(q, t, 0).start()

    def stage4(q):
        for t in range(2):
            for e in range(2):
                wait(u2(q, t, e), sem_u2.at[q % SLOTS, t, e])
            add(total(q, t), u2(q, t, 0), u2(q, t, 1), *cell(q, t, place[t][1]))

    def adamw(dst, w, m, v, g):
        w, g = w.astype(F32), g.astype(F32)
        m = 0.9 * m + 0.1 * g
        v = 0.95 * v + 0.05 * g * g
        step = m * lax.rsqrt(v + 1e-8) + 0.1 * w
        dst[...] = (w - 0.02 * step).astype(BF16)
        return m, v

    third, mid = pieces // 2, 24
    top, cut = pieces * ROWS // 2 - third * ROWS, 16

    def parts(core):
        return [((third + 1) * core + k, 0, pl.multiple_of(mid * core + ROWS * k, 8), ROWS) for k in range(third)] + [
            (third, pl.multiple_of(cut * core, 16), pl.multiple_of(third * ROWS * (1 - core), 8), mid)]

    mine = pl.ds((mid + third * ROWS - md.shape[0]) * c, md.shape[0])

    def loads_d():
        copies = [pltpu.make_async_copy(md, mbd.at[mine], sem_m.at[0, 0]), pltpu.make_async_copy(vd, vbd.at[mine], sem_m.at[1, 0])]
        rows = pl.ds(pl.multiple_of((third + 1) * ROWS * c, 8), third * ROWS)
        for t in range(2):
            copies.append(pltpu.make_async_copy(wd.at[t, x, y, rows], wb3.at[t], sem_m.at[2 + t, 0]))
            rest = pl.ds(pl.multiple_of(third * ROWS + cut * c, 8), mid)
            copies.append(pltpu.make_async_copy(wd.at[t, x, y, rest], wbm.at[t], sem_m.at[4 + t, 0]))
        return copies

    def swap_d(step):
        copies = []
        for t in range(2):
            if step == 0:
                three = (total_ref.at[pl.ds((third + 1) * other, third), t], got3.at[t])
                rest = (total(third, t).at[pl.ds(pl.multiple_of(cut * other, 16), mid)], gotm.at[t])
            else:
                three = (put3.at[other, t], new_ref.at[pl.ds((third + 1) * c, third), t])
                rest = (putm.at[other, t], newm.at[t])
            copies.append(send(*three, sem_xs.at[step, t, 0], sem_xr.at[step, t, 0], partner))
            copies.append(send(*rest, sem_xs.at[step, t, 1], sem_xr.at[step, t, 1], partner))
        return copies

    def step_d():
        for t in range(2):
            for k, (piece, r, row, size) in enumerate(parts(c)):
                for h in range(2):
                    g = (total(piece, t).at[pl.ds(r, size)], got3.at[t, k] if k < third else gotm.at[t])[h]
                    half = (c, other)[h]
                    dst = put3.at[half, t, k] if k < third else putm.at[half, t]
                    for b in range(COLS // 128):
                        lane = pl.ds(pl.multiple_of(half * COLS + 128 * b, 128), 128)
                        here = slice(128 * b, 128 * b + 128)
                        rows = pl.ds(row, size)
                        w = wb3[t, ROWS * k:ROWS * k + ROWS, lane] if k < third else wbm[t, :, lane]
                        mbd[rows, t, lane], vbd[rows, t, lane] = adamw(dst.at[:, here], w, mbd[rows, t, lane], vbd[rows, t, lane], g[:, here])

    def merge_d():
        for t in range(2):
            for k in range(third):
                new((third + 1) * c + k, t)[...] = put3[c, t, k]
            a, b = putm[c, t], newm[t]
            low, high = jnp.where(c == 0, a, b), jnp.where(c == 0, b, a)
            line = lax.broadcasted_iota(jnp.int32, (mid - cut, COLS), 0)
            new(third, t)[0:cut] = low[0:cut]
            new(third, t)[cut:mid] = jnp.where(line < top - cut, low[cut:mid].astype(F32), high[0:mid - cut].astype(F32)).astype(BF16)
            new(third, t)[mid:ROWS] = high[mid - cut:mid]

    def loads_g(w):
        (m, v), (mb, vb) = (((mg, vg), (mbg, vbg)), ((mu, vu), (mbu, vbu)))[w - 1]
        return [pltpu.make_async_copy(m, mb, sem_m.at[6, w - 1]), pltpu.make_async_copy(v, vb, sem_m.at[7, w - 1])]

    def load_w(w):
        return pltpu.make_async_copy((wg, wu)[w - 1].at[:, x, y, c], wbg, sem_m.at[8, w - 1])

    def step_g(w):
        mb, vb = ((mbg, vbg), (mbu, vbu))[w - 1]
        for t in range(2):
            for p in range(pieces):
                for b in range(COLS // 128):
                    here, lane = slice(128 * b, 128 * b + 128), slice(COLS * p + 128 * b, COLS * p + 128 * b + 128)
                    mb[t, :, lane], vb[t, :, lane] = adamw(
                        new(w * pieces + p, t).at[:, here], wbg[t, :, lane], mb[t, :, lane], vb[t, :, lane], total(w * pieces + p, t)[:, here])

    def piece(q, v):
        return kept.at[q - DIRECT] if v else whole.at[q]

    def block(q, t, i, j, v):
        a, b = at(t, i, j)
        return piece(q, v).at[t, c, a, b]

    def line(q, t, i, v, h=None):
        some = slice(None) if h is None else pl.ds(2 * h, 2)
        return piece(q, v).at[t, c, i % SIDE, some] if t == 0 else piece(q, v).at[t, c, some, i % SIDE]

    def across(q, t, i, v):
        send(line(q, t, i, v), line(q, t, i, v), sem_os.at[t], sem_or.at[q % TURNS, t], partner).start()

    def gather0(q, v):
        for t in range(2):
            i, j = place[t]
            for d in range(2):
                send(new(q, t), block(q, t, i, j, v), sem_gs.at[t, d], sem_gr.at[q % TURNS, t, d], dev_j(t, (1, 3)[d])).start()
            if v:
                block(q, t, i, j, v)[...] = new(q, t)[...]
            else:
                pltpu.make_async_copy(new(q, t), block(q, t, i, j, v), sem_own.at[t, q % 4]).start()

    def gather1(q, v):
        for t in range(2):
            i, j = place[t]
            wait(new(q, t), sem_gr.at[q % TURNS, t, 0])
            wait(new(q, t), sem_gr.at[q % TURNS, t, 1])
            src = block(q, t, i, j + side(q), v)
            send(src, src, sem_gs.at[t, 2], sem_gr.at[q % TURNS, t, 2], dev_j(t, SIDE - side(q))).start()
            if not v:
                wait(new(q, t), sem_own.at[t, q % 4])

    def gather2(q, v):
        for t in range(2):
            wait(new(q, t), sem_gr.at[q % TURNS, t, 2])
            for k in range(2):
                for d in range(2):
                    half = line(q, t, place[t][0], v, (d, 1 - d)[k])
                    send(half, half, sem_gs.at[t, 3 + 2 * k + d], sem_gr.at[q % TURNS, t, 3 + 2 * k + d], dev_i(t, (1, 3)[d])).start()
            across(q, t, place[t][0], v)

    def gather3(q, v):
        for t in range(2):
            for d in range(2):
                half = line(q, t, place[t][0] + (3, 1)[d], v, d)
                wait(half, sem_gr.at[q % TURNS, t, 3 + d])
                send(half, half, sem_gs.at[t, 7 + d], sem_gr.at[q % TURNS, t, 7 + d], dev_i(t, (1, 3)[d])).start()
        for t in range(2):
            for d in range(2):
                there = place[t][0] + (3, 1)[d]
                wait(line(q, t, there, v, 1 - d), sem_gr.at[q % TURNS, t, 5 + d])
                across(q, t, there, v)

    def gather4(q, v):
        for t in range(2):
            there = place[t][0] + 2
            for d in range(2):
                wait(line(q, t, there, v, d), sem_gr.at[q % TURNS, t, 7 + d])
            across(q, t, there, v)

    def keep(q, v):
        for t in range(2):
            wait(piece(q, v).at[t, other], sem_or.at[q % TURNS, t])
        if not v:
            @pl.when(q >= PULLED)
            def _():
                pltpu.make_async_copy(whole.at[q], kept.at[q - PULLED + count - DIRECT], sem_kept).start()

    def when(q, do):
        @pl.when(jnp.logical_and(q >= 0, q < count))
        def _():
            do(q)

    def each(q, do):
        for v in range(2):
            @pl.when(jnp.logical_and(q >= DIRECT * v, q < (DIRECT, count)[v]))
            def _(v=v):
                do(q, v == 1)

    def on(tick, t, do):
        @pl.when(t == tick)
        def _():
            do()

    load_own(0)
    barrier = pltpu.get_barrier_semaphore()
    peers = [dev(x + 1, y, c), dev(x + 3, y, c), dev(x, y + 1, c), dev(x, y + 3, c), partner]
    for peer in peers:
        pl.semaphore_signal(barrier, inc=1, device_id={"dp": peer}, device_id_type=MESH)
    pl.semaphore_wait(barrier, len(peers))
    for k in range(3):
        for t in range(2):
            chunk(t, k).start()
    swap(1)
    for t in range(2):
        chunk(t, 3).start()
    for q in range(2, AHEAD):
        swap(q)
    for copy in loads_d() + loads_g(1) + loads_g(2) + [load_w(1)]:
        copy.start()
    stage0_first()
    stage1(0)
    stage0_rest()

    ends = [w * pieces + pieces - 1 + LAG[4] for w in range(WEIGHTS)]
    gathers = ends[0] + 2
    clear = ends[-1] + 1
    stages = (stage0, stage1, stage2, stage3, stage4)
    rounds = (gather0, gather1, gather2, gather3, gather4, keep)
    assert PULLED + gathers + ROUND[5] > clear and kept.shape[0] == count - PULLED and count - DIRECT == HELD + 1

    def start(copies):
        for copy in copies:
            copy.start()

    def finish(copies):
        for copy in copies:
            copy.wait()

    def d_begin():
        start(swap_d(0))

    def d_step():
        finish(loads_d())
        finish(swap_d(0))
        step_d()
        start(swap_d(1))

    def d_end():
        finish(swap_d(1))
        merge_d()

    def g_step(w):
        finish(loads_g(w))
        load_w(w).wait()
        step_g(w)
        if w + 1 < WEIGHTS:
            load_w(w + 1).start()

    def sent():
        for z in range(SENT):
            for t in range(2):
                for d in range(2):
                    wait(s1(z, t, d), sem_s1.at[z, t, d])
                    wait(t2(z, t, d), sem_t2.at[z, t, d])
                    for h in range(2):
                        wait(s2(z, t, d, h), sem_s2.at[z, t, d, h])
                wait(t1(z, t), sem_t1.at[z, t])

    def cleared():
        sent()
        pl.semaphore_signal(sem_free, inc=1, device_id={"dp": partner}, device_id_type=MESH)

    def tick(t, _):
        when(t + AHEAD, swap)
        when(t + 1, load)
        on(DIRECT + gathers + ROUND[2], t, lambda: pl.semaphore_wait(sem_free, 1))
        for k in range(5, 0, -1):
            each(t - gathers - ROUND[k], rounds[k])
        for k in range(4, 1, -1):
            when(t - LAG[k], stages[k])

        @pl.when(t > LAG[1])
        def _():
            when(t - LAG[1], stage1)

        @pl.when(t > 0)
        def _():
            when(t, stage0)
        on(ends[0], t, d_begin)
        on(ends[0] + 1, t, d_step)
        on(ends[0] + 2, t, d_end)
        for w in range(1, WEIGHTS):
            on(ends[w], t, functools.partial(g_step, w))
        on(clear, t, cleared)
        each(t - gathers, gather0)
        return 0

    lax.fori_loop(0, count + gathers + ROUND[5], tick, 0)

    for t in range(2):
        wait(theirs.at[1:, t], sem_swap_s.at[t])
        for k in range(3):
            wait(theirs.at[:, t, 0, 0], sem_gs.at[t, k])
        for k in range(3, 9):
            wait(theirs.at[:, t, 0, 0:2], sem_gs.at[t, k])
        wait(theirs.at[:, t], sem_os.at[t])
    wait(kept.at[0:DIRECT - PULLED], sem_kept)


def put(pieces, slots, whole, kept, mbd, vbd, mbg, vbg, mbu, vbu, out_d, out_g, out_u, md, vd, mg, vg, mu, vu, buf, sem_in, sem_out, sem_kept, sem_m):
    steps = [(q, t, c) for q in range(PULLED) for t in range(2) for c in range(CORES)]
    rest = [(q, t, c) for q in range(PULLED, WEIGHTS * pieces) for t in range(2) for c in range(CORES)]

    def dst(q, t, c):
        w, p = divmod(q, pieces)
        if w == 0:
            return out_d.at[t, :, :, ROWS * p:ROWS * p + ROWS, COLS * c:COLS * c + COLS]
        return (out_g, out_u)[w - 1].at[t, :, :, c, :, COLS * p:COLS * p + COLS]

    def load(s):
        return pltpu.make_async_copy(whole.at[steps[s]], buf.at[s % slots], sem_in.at[s % slots])

    def store(s):
        return pltpu.make_async_copy(buf.at[s % slots], dst(*steps[s]), sem_out.at[s % slots])

    mine = pl.ds((mbd.shape[0] - md.shape[0]) * (lax.axis_index("dp") % CORES), md.shape[0])
    moments = [(mbd.at[mine], md), (vbd.at[mine], vd), (mbg, mg), (vbg, vg), (mbu, mu), (vbu, vu)]
    moments = [pltpu.make_async_copy(src, dst, sem_m.at[k]) for k, (src, dst) in enumerate(moments)]
    ahead = slots // 2
    for s in range(ahead):
        load(s).start()
    for copy in moments:
        copy.start()
    for s in range(len(steps)):
        for q, t, c in rest[len(rest) * s // len(steps):len(rest) * (s + 1) // len(steps)]:
            slot = q - DIRECT if q >= DIRECT else q - PULLED + WEIGHTS * pieces - DIRECT
            pltpu.make_async_copy(kept.at[slot, t, c], dst(q, t, c), sem_kept).start()
        if s + ahead < len(steps):
            if s + ahead >= slots:
                store(s + ahead - slots).wait()
            load(s + ahead).start()
        load(s).wait()
        store(s).start()
    for s in range(max(0, len(steps) - slots), len(steps)):
        store(s).wait()
    pltpu.make_async_copy(kept, kept, sem_kept).wait()
    for copy in moments:
        copy.wait()


def solution(mesh):
    devices = mesh.shape["dp"]
    assert devices == CORES * SIDE * SIDE

    def step(*arrays):
        (gg, gu, gd), (wg, wu, wd), (mg, mu, md), (vg, vu, vd) = (arrays[i : i + 3] for i in (0, 3, 6, 9))
        layers, rows, wide = wg.shape
        tall, narrow = wd.shape[1:]
        pieces = wide // COLS
        chip = tall // (SIDE * SIDE)
        assert layers == 2 and rows == devices * ROWS and narrow == CORES * COLS and chip == pieces * ROWS
        split_g = (layers, SIDE, SIDE, CORES, ROWS, wide)
        split_d = (layers, SIDE, SIDE, chip, narrow)
        block = (ROWS, COLS)
        count = WEIGHTS * pieces
        hbm, vmem = pl.BlockSpec(memory_space=pltpu.HBM), pl.BlockSpec(memory_space=pltpu.VMEM)
        dma = pltpu.SemaphoreType.DMA
        third, mid = pieces // 2, 24
        window = third * ROWS + mid
        md, vd = (a.transpose(1, 0, 2) for a in (md, vd))
        whole, kept, _, *moments = pl.pallas_call(
            functools.partial(fused, pieces),
            out_shape=(
                jax.ShapeDtypeStruct((DIRECT, 2, CORES, SIDE, SIDE, *block), BF16),
                pltpu.VMEM((count - PULLED, 2, CORES, SIDE, SIDE, *block), BF16),
                jax.ShapeDtypeStruct((count, 2, SIDE, SIDE, *block), BF16),
                *(pltpu.VMEM((window, *md.shape[1:]), F32) for _ in range(2)),
                *(pltpu.VMEM(mg.shape, F32) for _ in range(4)),
            ),
            in_specs=[hbm] * 12,
            out_specs=[hbm, vmem, hbm] + [vmem] * 6,
            scratch_shapes=[
                pltpu.VMEM((count, 2, *block), BF16),
                pltpu.VMEM((count, 2, *block), BF16),
                pltpu.VMEM((2, third, *block), BF16),
                pltpu.VMEM((2, mid, COLS), BF16),
                pltpu.VMEM((CORES, 2, third, *block), BF16),
                pltpu.VMEM((CORES, 2, mid, COLS), BF16),
                pltpu.VMEM((2, mid, COLS), BF16),
                pltpu.VMEM((layers, third * ROWS, narrow), BF16),
                pltpu.VMEM((layers, mid, narrow), BF16),
                pltpu.VMEM((layers, ROWS, wide), BF16),
                dma((2, 2, 2)),
                dma((2, 2, 4)),
                dma((2,)),
                dma((TURNS, 2)),
                dma((SLOTS, 2, 2)),
                dma((SLOTS, 2, 2, 2)),
                dma((SLOTS, 2)),
                dma((SLOTS, 2, 2)),
                dma((SENT, 2, 2)),
                dma((SENT, 2, 2, 2)),
                dma((SENT, 2)),
                dma((SENT, 2, 2)),
                dma((9, 2)),
                dma((2, 2, 2)),
                dma((2, 2, 2)),
                dma((2, 4)),
                dma((2, 9)),
                dma((TURNS, 2, 9)),
                dma((2,)),
                dma((TURNS, 2)),
                dma,
                pltpu.SemaphoreType.REGULAR,
            ],
            name="fused",
            compiler_params=pltpu.CompilerParams(collective_id=0, has_side_effects=True, vmem_limit_bytes=8 * 2**20),
        )(
            gd.reshape(split_d), gg.reshape(split_g), gu.reshape(split_g), wd.reshape(split_d), wg.reshape(split_g), wu.reshape(split_g),
            md, vd, mg, vg, mu, vu,
        )
        slots = 9
        new_d, new_g, new_u, md, vd, mg, vg, mu, vu = pl.pallas_call(
            functools.partial(put, pieces, slots),
            out_shape=(*(jax.ShapeDtypeStruct(s, BF16) for s in (split_d, split_g, split_g)), *(jax.ShapeDtypeStruct(a.shape, F32) for a in (md, vd, mg, vg, mu, vu))),
            in_specs=[hbm] + [vmem] * 7,
            out_specs=[hbm] * 9,
            scratch_shapes=[pltpu.VMEM((slots, SIDE, SIDE, *block), BF16), dma((slots,)), dma((slots,)), dma, dma((6,))],
            name="put",
            compiler_params=pltpu.CompilerParams(vmem_limit_bytes=8 * 2**20),
        )(whole, *(pltpu.with_memory_space_constraint(a, pltpu.VMEM) for a in (kept, *moments)))
        md, vd = (a.transpose(1, 0, 2) for a in (md, vd))
        return (new_g.reshape(wg.shape), new_u.reshape(wu.shape), new_d.reshape(wd.shape), mg, mu, md, vg, vu, vd)

    all_of, cut = P(None, None, None), P(None, "dp", None)
    return jax.shard_map(
        step,
        mesh=mesh,
        in_specs=(P(("rep", "dp"), None, None, None),) * 3 + (all_of,) * 3 + (cut,) * 6,
        out_specs=(P("rep", None, None),) * 3 + (P("rep", "dp", None),) * 6,
        check_vma=False,
    )
```
